32 devices in a mesh: rep: 1, dp: 32 (over x, y, z, core).
Axes of the slice: x: 2, y: 2, z: 4, core: 2. Of those that a mesh axis runs over, the one named last changes fastest.
Arguments:
- x: bfloat16 [32, 2048, 1024], P(('rep', 'dp'))
- dy: bfloat16 [32, 2048, 1024], P(('rep', 'dp'))
- w_gate: bfloat16 [2, 1024, 3328], replicated
- w_up: bfloat16 [2, 1024, 3328], replicated
- w_down: bfloat16 [2, 3328, 1024], replicated
- m_w_gate: float32 [2, 1024, 3328], P(None, 'dp')
- m_w_up: float32 [2, 1024, 3328], P(None, 'dp')
- m_w_down: float32 [2, 3328, 1024], P(None, 'dp')
- v_w_gate: float32 [2, 1024, 3328], P(None, 'dp')
- v_w_up: float32 [2, 1024, 3328], P(None, 'dp')
- v_w_down: float32 [2, 3328, 1024], P(None, 'dp')
Outputs:
- output 1: bfloat16 [2, 1024, 3328], P('rep')
- output 2: bfloat16 [2, 1024, 3328], P('rep')
- output 3: bfloat16 [2, 3328, 1024], P('rep')
- output 4: float32 [2, 1024, 3328], P('rep', 'dp')
- output 5: float32 [2, 1024, 3328], P('rep', 'dp')
- output 6: float32 [2, 3328, 1024], P('rep', 'dp')
- output 7: float32 [2, 1024, 3328], P('rep', 'dp')
- output 8: float32 [2, 1024, 3328], P('rep', 'dp')
- output 9: float32 [2, 3328, 1024], P('rep', 'dp')
All inputs are finite; a program needn't handle non-finite values.
Results may differ from the reference program's by a relative error of at most 0.022.
Values are sent between devices in bfloat16 or wider.
A program may use at most 2 GiB of HBM per device.

```python
import jax
import jax.numpy as jnp
from jax import lax

SEQUENCES = 32
TOKENS = 2048
D = 1024
FF = 3328
LAYERS = 2
NAMES = ("w_gate", "w_up", "w_down")
SHAPES = {"w_gate": (LAYERS, D, FF), "w_up": (LAYERS, D, FF), "w_down": (LAYERS, FF, D)}


def bump(key, n, height):
    away = (jnp.arange(n, dtype=jnp.int32) - jax.random.randint(key, (), 0, n, jnp.int32)) % n
    return jnp.where(away < n // 8, height, 1.0)


def together(key, own, strength):
    shared = jax.random.normal(key, own.shape[1:], jnp.float32)
    return (own + strength * shared) * lax.rsqrt(1 + strength * strength)


def setup_inputs(seed: int = 0, part: int = 0) -> dict:
    kx, kdy, ka, kb, kz, kf, kh, kl, *keys = jax.random.split(jax.random.key(seed), 8 + 3 * len(NAMES))
    kx, kdy, ka, kb = (jax.random.fold_in(k, part) for k in (kx, kdy, ka, kb))
    kw, km, kv = (keys[i::3] for i in range(3))
    shape = (SEQUENCES, TOKENS, D)
    much_x, much_dy = jax.random.uniform(kz, (2,), jnp.float32, 0.0, 1.0)
    loud = 2.0 ** jax.random.uniform(jax.random.fold_in(kz, 1), (), jnp.float32, -1.0, 2.0)
    layers = 2.0 ** jax.random.uniform(kl, (LAYERS, 1, 1), jnp.float32, -1.0, 1.0)
    x = together(ka, jax.random.normal(kx, shape, jnp.float32), much_x) * bump(kf, D, 4.0)
    dy = together(kb, jax.random.normal(kdy, shape, jnp.float32), much_dy)
    drawn = {"x": x.astype(jnp.bfloat16), "dy": (loud * dy * (SEQUENCES * TOKENS) ** -0.5).astype(jnp.bfloat16)}
    for key, name in zip(kw, NAMES, strict=True):
        w = jax.random.normal(key, SHAPES[name], jnp.float32) * SHAPES[name][1] ** -0.5
        drawn[name] = (w * {"w_gate": 1.0, "w_up": bump(kh, FF, 4.0), "w_down": layers}[name]).astype(jnp.bfloat16)
    for key, name in zip(km, NAMES, strict=True):
        drawn[f"m_{name}"] = 0.1 * jax.random.normal(key, SHAPES[name], jnp.float32)
    for key, name in zip(kv, NAMES, strict=True):
        drawn[f"v_{name}"] = jax.random.uniform(key, SHAPES[name], jnp.float32, 0.005, 0.015)
    return drawn


def matmul(a, w):
    return jnp.dot(a, w, preferred_element_type=jnp.float32).astype(jnp.bfloat16)


def normed(h):
    wide = h.astype(jnp.float32)
    scale = lax.rsqrt(jnp.mean(wide**2, -1, keepdims=True) + 1e-6)
    return (wide * scale).astype(jnp.bfloat16)


def layer(h, w):
    a = normed(h)
    gate = jnp.dot(a, w["w_gate"], preferred_element_type=jnp.float32)
    up = jnp.dot(a, w["w_up"], preferred_element_type=jnp.float32)
    return h + matmul((jax.nn.silu(gate) * up).astype(jnp.bfloat16), w["w_down"])


def adamw(w, m, v, g):
    m = 0.9 * m + 0.1 * g
    v = 0.95 * v + 0.05 * g * g
    step = m * lax.rsqrt(v + 1e-8) + 0.1 * w
    return (w - 0.02 * step).astype(jnp.bfloat16), m, v


def clipped(gradients, sum_of_squares, count):
    factor = jnp.minimum(1.0, 0.5 * lax.rsqrt(sum_of_squares / count + 1e-30))
    return [g * factor for g in gradients]


def stack(weights, h):
    return lax.scan(lambda h, w: (layer(h, w), None), h, weights)[0]


def reference(x, dy, w_gate, w_up, w_down, m_w_gate, m_w_up, m_w_down, v_w_gate, v_w_up, v_w_down):
    weights = dict(zip(NAMES, (w_gate, w_up, w_down), strict=True))

    def take(so_far, sequence):
        h, by_y = sequence
        _, back = jax.vjp(lambda w: stack(w, h), weights)
        return jax.tree.map(lambda total, term: total + term.astype(jnp.float32), so_far, back(by_y)[0]), None

    none_yet = {name: jnp.zeros(w.shape, jnp.float32) for name, w in weights.items()}
    by_weights, _ = lax.scan(take, none_yet, (x, dy))
    gradients = [by_weights[name].astype(jnp.bfloat16).astype(jnp.float32) for name in NAMES]
    gradients = clipped(gradients, sum(jnp.sum(g * g) for g in gradients), sum(g.size for g in gradients))
    new = [
        adamw(w.astype(jnp.float32), m, v, g)
        for w, m, v, g in zip((w_gate, w_up, w_down), (m_w_gate, m_w_up, m_w_down), (v_w_gate, v_w_up, v_w_down), gradients, strict=True)
    ]
    return tuple(one[which] for which in range(3) for one in new)
```

```python
import jax
import jax.numpy as jnp
from jax import lax
from jax.experimental import pallas as pl
from jax.experimental.pallas import tpu as pltpu
from jax.sharding import PartitionSpec as P

BF, F32 = jnp.bfloat16, jnp.float32
MESH = pl.DeviceIdType.MESH

BITS = {"x": 0, "y": 1, "zh": 2, "zl": 3, "c": 4}

ROUTE = ("A", "A", "B", "B", "Cx", "Cy")
END = (65, 36, 8, 81, 52, 24, 1, 84, 72, 17, 4, 40, 33, 20, 56, 49, 68, 88, 69, 73, 12, 44, 66, 37, 9, 85, 89, 28, 60, 82, 53, 92, 25, 5, 76, 41, 2, 21, 57, 18, 74, 45, 77, 70, 34, 13, 50, 93, 86, 90, 29, 61, 67, 38, 10, 6, 42, 58, 22, 78, 83, 54, 26, 94, 75, 71, 14, 46, 3, 19, 91, 62, 87, 30, 35, 79, 51, 95, 43, 7, 39, 11, 23, 59, 15, 47, 55, 27, 31, 63)
MID = (65, 66, 36, 8, 81, 82, 52, 24, 1, 2, 84, 72, 17, 18, 4, 40, 33, 34, 20, 56, 49, 50, 68, 88, 37, 9, 67, 69, 73, 38, 70, 74, 10, 12, 44, 53, 25, 83, 85, 89, 54, 86, 90, 26, 28, 60, 3, 92, 5, 19, 6, 76, 41, 42, 35, 51, 21, 57, 22, 58, 39, 11, 45, 13, 75, 46, 55, 27, 71, 77, 14, 78, 61, 29, 91, 93, 62, 94, 87, 30, 7, 43, 23, 59, 15, 47, 63, 31, 79, 95)

def at(x, y, z, c):
    return ((x * 2 + y) * 4 + z) * 2 + c

class Place:
    def __init__(self):
        me = lax.axis_index("dp")
        self.me = me
        self.x, self.y, self.z, self.c = x, y, z, c = me // 16, me // 8 % 2, me // 2 % 4, me % 2
        self.end = (z == 0) | (z == 3)
        low = z < 2
        self.planes = (z, jnp.where(z == 0, 1, jnp.where(z == 1, 0, jnp.where(z == 2, 3, 2))), jnp.where(low, 2, 1), jnp.where(low, 3, 0))
        inner = jnp.where(z == 0, 1, jnp.where(z == 1, 2, jnp.where(z == 2, 1, 2)))
        outer = jnp.where(low, 0, 3)
        self.to = {"x": at(1 - x, y, z, c), "y": at(x, 1 - y, z, c), "core": at(x, y, z, 1 - c), "in": at(x, y, inner, c), "out": at(x, y, outer, c)}

    def chip(self, dx, dy, s):
        x = 1 - self.x if dx else self.x
        y = 1 - self.y if dy else self.y
        return (x * 2 + y) * 4 + self.planes[s]

def onward(route, dx, dy, s, end):
    z = {0: ["in"] if end else ["out", "in"], 1: [] if end else ["in"], 2: [] if end else ["out"], 3: [] if end else ["out"]}[s]
    own = (dx, dy, s) == (0, 0, 0)
    first, second = ("x", "y") if route in ("A", "Cx") else ("y", "x")
    near = dy == 0 if first == "x" else dx == 0
    side = dx if first == "x" else dy
    if route in "AB":
        if own: return [first, *z, second]
        if not near: return []
        return [*z, second]
    if not near: return []
    if side: return [second]
    return [*z, first, second]

def signal(sem, device):
    pl.semaphore_signal(sem, inc=1, device_id={"dp": device}, device_id_type=MESH)

def entry(here):
    sem = pltpu.get_barrier_semaphore()
    for link in ("x", "y", "core", "in"): signal(sem, here.to[link])
    @pl.when(jnp.logical_not(here.end))
    def _(): signal(sem, here.to["out"])
    pl.semaphore_wait(sem, jnp.where(here.end, 4, 5))

def START(end):
    zz = ["in"] if end else ["out", "in"]
    A, B, X, Y = (0, 1), (2, 3), (4,), (5,)
    o = [(p, l) for p in X + Y for l in zz]
    o += [(p, "x") for p in A] + [(p, "y") for p in B] + [(p, l) for p in A + B for l in zz]
    o += [(p, "x") for p in X] + [(p, "y") for p in Y] + [(p, "x") for p in B + Y] + [(p, "y") for p in A + X]
    return o + [(p, "core") for p in range(6)]

def gather_refs(here, outs, sends, link, core):
    def region(p, owner):
        ref = outs[p // 2]
        rows = ref.shape[1] // 32
        return ref.at[p % 2, pl.ds(pl.multiple_of(owner * rows, 8), rows), :]
    def run(end):
        started = []
        def send(p, chip, to):
            r = region(p, chip * 2 + here.c)
            cp = pltpu.make_async_remote_copy(r, r, sends.at[len(started)], (core if to == "core" else link).at[p, chip], device_id={"dp": here.to[to]}, device_id_type=MESH)
            started.append(cp)
            cp.start()
        def wait(p, owner, sem):
            pltpu.make_async_copy(region(p, owner), region(p, owner), sem).wait()
        mine = here.chip(0, 0, 0)
        for p, to in START(end): send(p, mine, to)
        for code in END if end else MID:
            p, dx, dy, s = code // 16, code // 8 % 2, code // 4 % 2, code % 4
            chip = here.chip(dx, dy, s)
            wait(p, chip * 2 + here.c, link.at[p, chip])
            for to in onward(ROUTE[p], dx, dy, s, end) + ["core"]: send(p, chip, to)
        def landed(chip, _):
            for p in range(6): wait(p, chip * 2 + 1 - here.c, core.at[p, chip])
            return 0
        lax.fori_loop(0, 16, landed, 0)
        for cp in started: cp.wait_send()
    @pl.when(here.end)
    def _(): run(True)
    @pl.when(jnp.logical_not(here.end))
    def _(): run(False)


def scatter(g, order):
    me = lax.axis_index("dp")
    rows = g.shape[0] // 32
    own = {k: me // 2 ** (4 - n) % 2 for k, n in BITS.items()}
    terms = [((), g.reshape(2, 2, 2, 2, 2, rows, g.shape[1]))]

    def part(gone, a, bits):
        left = [k for k in BITS if k not in gone]
        starts = [bits.get(k, 0) for k in left] + [0, 0]
        sizes = [1 if k in bits else 2 for k in left] + list(a.shape[-2:])
        a = lax.dynamic_slice(a, starts, sizes)
        return a.reshape([2 for k in left if k not in bits] + list(a.shape[-2:])).astype(F32)

    done = {}
    for k in ("c", *order):
        pick = {**done, k: 1 - own[k]}
        send = sum(part(gone, a, {b: i for b, i in pick.items() if b not in gone}) for gone, a in terms).astype(BF)
        flip = 2 ** (4 - BITS[k])
        got = lax.ppermute(send, "dp", [(d, d ^ flip) for d in range(32)])
        done[k] = own[k]
        terms.append((tuple(done), got))
    total = sum(part(gone, a, {b: i for b, i in done.items() if b not in gone}) for gone, a in terms)
    return total.astype(BF)

def gather(*own, collective_id=1):
    outs = [jax.ShapeDtypeStruct((2, 32 * o.shape[1], o.shape[2]), o.dtype) for o in own]
    def kern(*refs):
        own, outs, stage = refs[:3], refs[3:6], refs[6:9]
        ssem, sends, link, core = refs[9:]
        here = Place()
        for p in range(6):
            pltpu.make_async_copy(own[p // 2].at[p % 2], stage[p // 2].at[p % 2], ssem.at[p]).start()
        entry(here)
        cps = []
        for p in range(6):
            pltpu.make_async_copy(own[p // 2].at[p % 2], stage[p // 2].at[p % 2], ssem.at[p]).wait()
            rows = stage[p // 2].shape[1]
            cp = pltpu.make_async_copy(stage[p // 2].at[p % 2], outs[p // 2].at[p % 2, pl.ds(pl.multiple_of(here.me * rows, 8), rows), :], ssem.at[p]); cp.start(); cps.append(cp)
        for cp in cps: cp.wait()
        gather_refs(here, outs, sends, link, core)
    return pl.pallas_call(kern, out_shape=outs, in_specs=[pl.BlockSpec(memory_space=pl.ANY)] * 3, out_specs=[pl.BlockSpec(memory_space=pl.ANY)] * 3,
        scratch_shapes=[pltpu.VMEM(o.shape, o.dtype) for o in own] + [pltpu.SemaphoreType.DMA((6,)), pltpu.SemaphoreType.DMA((240,)), pltpu.SemaphoreType.DMA((6, 16)), pltpu.SemaphoreType.DMA((6, 16))],
        name="gather", compiler_params=pltpu.CompilerParams(collective_id=collective_id, has_side_effects=True, vmem_limit_bytes=8 << 20))(*own)


def dot(a, b, contract):
    return lax.dot_general(a, b, ((contract[:1], contract[1:]), ((), ())), preferred_element_type=F32)


def normed(h):
    wide = h.astype(F32)
    scale = lax.rsqrt(jnp.mean(wide**2, -1, keepdims=True) + 1e-6)
    return (wide * scale).astype(BF), scale


def gates(gate, up, by_hidden):
    by = by_hidden.astype(F32)
    sigmoid = jax.nn.sigmoid(gate)
    by_gate = by * up * (sigmoid * (1 + gate * (1 - sigmoid)))
    return by_gate.astype(BF), (by * gate * sigmoid).astype(BF)


def adamw(w, m, v, g):
    m = 0.9 * m + 0.1 * g
    v = 0.95 * v + 0.05 * g * g
    step = m * lax.rsqrt(v + 1e-8) + 0.1 * w
    return (w - 0.02 * step).astype(BF), m, v


def solution(mesh):
    ORDERS = (("x", "y", "zl", "zh"), ("y", "x", "zl", "zh"), ("zl", "x", "y", "zh"), ("x", "y", "zl", "zh"), ("y", "x", "zl", "zh"), ("zl", "y", "x", "zh"))
    def step(x, dy, *arrays):
        orders = iter(ORDERS)
        w, m, v = (arrays[i : i + 3] for i in (0, 3, 6))
        h0, by_y = x[0], dy[0]
        layers = w[0].shape[0]
        h, kept = h0, []
        for n in range(layers):
            a, scale = normed(h)
            gate, up = dot(a, w[0][n], (1, 0)), dot(a, w[1][n], (1, 0))
            hidden = (jax.nn.silu(gate) * up).astype(BF)
            kept.append((h, a, scale, gate, up, hidden))
            if n + 1 < layers:
                h = h + dot(hidden, w[2][n], (1, 0)).astype(BF)
        sums = [[None] * layers for _ in range(3)]
        by = by_y
        for n in reversed(range(layers)):
            h, a, scale, gate, up, hidden = kept[n]
            sums[2][n] = scatter(dot(hidden, by, (0, 0)).astype(BF), next(orders))
            by_hidden = dot(by, w[2][n], (1, 1)).astype(BF)
            by_gate, by_up = gates(gate, up, by_hidden)
            sums[0][n] = scatter(dot(a, by_gate, (0, 0)).astype(BF), next(orders))
            sums[1][n] = scatter(dot(a, by_up, (0, 0)).astype(BF), next(orders))
            if n:
                by_a = dot(by_gate, w[0][n], (1, 1)).astype(BF) + dot(by_up, w[1][n], (1, 1)).astype(BF)
                wide, by_a = h.astype(F32), by_a.astype(F32)
                inner = jnp.mean(by_a * wide, -1, keepdims=True)
                by = by + (by_a * scale - wide * (scale**3 * inner)).astype(BF)
        g = [jnp.stack(s).astype(F32) for s in sums]
        squares = lax.psum(sum(jnp.sum(t * t) for t in g), "dp")
        count = sum(t.size for t in w)
        factor = jnp.minimum(1.0, 0.5 * lax.rsqrt(squares / count + 1e-30))
        me = lax.axis_index("dp")
        outs = []
        for w_, m_, v_, g_ in zip(w, m, v, g, strict=True):
            own = lax.dynamic_slice_in_dim(w_, me * m_.shape[1], m_.shape[1], 1)
            outs.append(adamw(own.astype(F32), m_, v_, g_ * factor))
        new = gather(*(o[0] for o in outs))
        return (*new, *(o[1] for o in outs), *(o[2] for o in outs))

    rows = P(None, "dp", None)
    return jax.shard_map(
        step,
        mesh=mesh,
        in_specs=(P(("rep", "dp")), P(("rep", "dp")), *(P(),) * 3, *(rows,) * 6),
        out_specs=(*(P("rep"),) * 3, *(P("rep", "dp", None),) * 6),
        check_vma=False,
    )
```

```python
import jax
import jax.numpy as jnp
from jax import lax
from jax.experimental import pallas as pl
from jax.experimental.pallas import tpu as pltpu
from jax.sharding import PartitionSpec as P

BF, F32 = jnp.bfloat16, jnp.float32
MESH = pl.DeviceIdType.MESH

ROUTE = ("A", "A", "B", "B", "Cx", "Cy")
END = (65, 36, 8, 81, 52, 24, 1, 84, 72, 17, 4, 40, 33, 20, 56, 49, 68, 88, 69, 73, 12, 44, 66, 37, 9, 85, 89, 28, 60, 82, 53, 92, 25, 5, 76, 41, 2, 21, 57, 18, 74, 45, 77, 70, 34, 13, 50, 93, 86, 90, 29, 61, 67, 38, 10, 6, 42, 58, 22, 78, 83, 54, 26, 94, 75, 71, 14, 46, 3, 19, 91, 62, 87, 30, 35, 79, 51, 95, 43, 7, 39, 11, 23, 59, 15, 47, 55, 27, 31, 63)
MID = (65, 66, 36, 8, 81, 82, 52, 24, 1, 2, 84, 72, 17, 18, 4, 40, 33, 34, 20, 56, 49, 50, 68, 88, 37, 9, 67, 69, 73, 38, 70, 74, 10, 12, 44, 53, 25, 83, 85, 89, 54, 86, 90, 26, 28, 60, 3, 92, 5, 19, 6, 76, 41, 42, 35, 51, 21, 57, 22, 58, 39, 11, 45, 13, 75, 46, 55, 27, 71, 77, 14, 78, 61, 29, 91, 93, 62, 94, 87, 30, 7, 43, 23, 59, 15, 47, 63, 31, 79, 95)

def at(x, y, z, c):
    return ((x * 2 + y) * 4 + z) * 2 + c

class Place:
    def __init__(self):
        me = lax.axis_index("dp")
        self.me = me
        self.x, self.y, self.z, self.c = x, y, z, c = me // 16, me // 8 % 2, me // 2 % 4, me % 2
        self.end = (z == 0) | (z == 3)
        low = z < 2
        self.planes = (z, jnp.where(z == 0, 1, jnp.where(z == 1, 0, jnp.where(z == 2, 3, 2))), jnp.where(low, 2, 1), jnp.where(low, 3, 0))
        inner = jnp.where(z == 0, 1, jnp.where(z == 1, 2, jnp.where(z == 2, 1, 2)))
        outer = jnp.where(low, 0, 3)
        self.own = {"x": x, "y": y, "zh": z // 2, "zl": z % 2, "c": c}
        self.to = {"zl": at(x, y, z + 1 - 2 * (z % 2), c), "zh": at(x, y, (z + 2) % 4, c), "x": at(1 - x, y, z, c), "y": at(x, 1 - y, z, c), "core": at(x, y, z, 1 - c), "in": at(x, y, inner, c), "out": at(x, y, outer, c)}

    def chip(self, dx, dy, s):
        x = 1 - self.x if dx else self.x
        y = 1 - self.y if dy else self.y
        return (x * 2 + y) * 4 + self.planes[s]

def onward(route, dx, dy, s, end):
    z = {0: ["in"] if end else ["out", "in"], 1: [] if end else ["in"], 2: [] if end else ["out"], 3: [] if end else ["out"]}[s]
    own = (dx, dy, s) == (0, 0, 0)
    first, second = ("x", "y") if route in ("A", "Cx") else ("y", "x")
    near = dy == 0 if first == "x" else dx == 0
    side = dx if first == "x" else dy
    if route in "AB":
        if own: return [first, *z, second]
        if not near: return []
        return [*z, second]
    if not near: return []
    if side: return [second]
    return [*z, first, second]

def signal(sem, device):
    pl.semaphore_signal(sem, inc=1, device_id={"dp": device}, device_id_type=MESH)

def START(end):
    zz = ["in"] if end else ["out", "in"]
    A, B, X, Y = (0, 1), (2, 3), (4,), (5,)
    o = [(p, l) for p in X + Y for l in zz]
    o += [(p, "x") for p in A] + [(p, "y") for p in B] + [(p, l) for p in A + B for l in zz]
    o += [(p, "x") for p in X] + [(p, "y") for p in Y] + [(p, "x") for p in B + Y] + [(p, "y") for p in A + X]
    return o + [(p, "core") for p in range(6)]

def gather_refs(here, outs, sends, link, core):
    def region(p, owner):
        ref = outs[p // 2]
        rows = ref.shape[1] // 32
        return ref.at[p % 2, pl.ds(pl.multiple_of(owner * rows, 8), rows), :]
    def run(end):
        started = []
        def send(p, chip, to):
            r = region(p, chip * 2 + here.c)
            cp = pltpu.make_async_remote_copy(r, r, sends.at[len(started)], (core if to == "core" else link).at[p, chip], device_id={"dp": here.to[to]}, device_id_type=MESH)
            started.append(cp)
            cp.start()
        def wait(p, owner, sem):
            pltpu.make_async_copy(region(p, owner), region(p, owner), sem).wait()
        mine = here.chip(0, 0, 0)
        for p, to in START(end): send(p, mine, to)
        for code in END if end else MID:
            p, dx, dy, s = code // 16, code // 8 % 2, code // 4 % 2, code % 4
            chip = here.chip(dx, dy, s)
            wait(p, chip * 2 + here.c, link.at[p, chip])
            for to in onward(ROUTE[p], dx, dy, s, end) + ["core"]: send(p, chip, to)
        def landed(chip, _):
            for p in range(6): wait(p, chip * 2 + 1 - here.c, core.at[p, chip])
            return 0
        lax.fori_loop(0, 16, landed, 0)
        for cp in started: cp.wait_send()
    @pl.when(here.end)
    def _(): run(True)
    @pl.when(jnp.logical_not(here.end))
    def _(): run(False)


XY, YX, ZX, ZY = ("x", "y", "zl", "zh"), ("y", "x", "zl", "zh"), ("zl", "x", "y", "zh"), ("zl", "y", "x", "zh")
WEIGHT = {"x": 8, "y": 4, "zh": 2, "zl": 1}
EVENTS = (1, 9, 17, 25, 33, 41, 2, 49, 10, 57, 18, 65, 26, 42, 34, 3, 66, 50, 4, 11, 5, 58, 19, 12, 27, 13, 35, 43, 28, 67, 36, 29, 51, 37, 59, 20, 44, 68, 52, 60, 21, 45, 69, 53, 61)


def streams(mats):
    out = []
    for m, ref in enumerate(mats):
        tiles = ref.shape[-1] // 128
        a, b = 128 * -(-tiles // 3), 128 * (-(-tiles // 3) + -(-(tiles - -(-tiles // 3)) // 2))
        out += [(m, 0, a, XY), (m, a, b - a, YX), (m, b, 128 * tiles - b, ZY if m % 2 else ZX)]
    return out


def sum_scratch(mats):
    out = []
    for m, _, w, _ in streams(mats):
        rows = mats[m].shape[-2]
        out += [pltpu.VMEM((16, rows, w), BF), pltpu.VMEM((31, rows, w), BF), pltpu.VMEM((15, rows, w), BF)]
    n = len(streams(mats))
    return [*out, pltpu.SemaphoreType.DMA((n,)), pltpu.SemaphoreType.DMA((n, 5)), pltpu.SemaphoreType.DMA((n, 5))]


class Sum:
    def __init__(self, here, mats, outs, scratch):
        self.here, self.mats, self.outs = here, mats, outs
        self.streams = streams(mats)
        n = len(self.streams)
        self.held = [scratch[3 * s : 3 * s + 3] for s in range(n)]
        self.local, self.sent, self.got = scratch[3 * n :]
        self.copies = {}

    def part(self, s, core):
        m, first, w, _ = self.streams[s]
        return self.mats[m].at[:, core, :, first : first + w]

    def send(self, s, j):
        here = self.here
        own, came, goes = self.held[s]
        order = ("core", *self.streams[s][3])
        n = 16 >> j
        src = self.part(s, 1 - here.c) if j == 0 else goes.at[16 - 2 * n : 16 - n]
        cp = pltpu.make_async_remote_copy(src, came.at[32 - 2 * n : 32 - n], self.sent.at[s, j], self.got.at[s, j], device_id={"dp": here.to[order[j]]}, device_id_type=MESH)
        self.copies[s, j] = cp
        cp.start()

    def start(self):
        for s in range(len(self.streams)):
            self.send(s, 0)
            pltpu.make_async_copy(self.part(s, self.here.c), self.held[s][0], self.local.at[s]).start()

    def event(self, code):
        s, j = code // 8, code % 8
        m, first, w, order = self.streams[s]
        own, came, goes = self.held[s]
        mine = self.here.own
        if j == 1:
            pltpu.make_async_copy(self.part(s, self.here.c), own, self.local.at[s]).wait()
        self.copies[s, j - 1].wait_recv()
        away = 0 if j == 5 else 1 - mine[order[j - 1]]

        def block(k):
            b = sum(mine[o] * WEIGHT[o] for o in order[: j - 1])
            if j < 5:
                b = b + away * WEIGHT[order[j - 1]]
            b = b + sum(k // 2 ** (3 - i) % 2 * WEIGHT[order[i]] for i in range(j, 4))
            total = own[b].astype(F32) + came[b].astype(F32)
            for i in range(1, j):
                at_i = 32 - (32 >> i) + sum(mine[order[t]] * 2 ** (3 - t) for t in range(i, j - 1)) + k
                if j < 5:
                    at_i = at_i + away * 2 ** (4 - j)
                total = total + came[at_i].astype(F32)
            return total.astype(BF)

        if j == 5:
            self.outs[m][:, first : first + w] = block(0)
            return
        n = 16 >> j

        def one(k, _):
            goes[16 - 2 * n + k] = block(k)
            return 0

        lax.fori_loop(0, n, one, 0)
        self.send(s, j)

    def finish(self):
        for cp in self.copies.values():
            cp.wait_send()


def entry(here):
    sem = pltpu.get_barrier_semaphore()
    for link in ("x", "y", "core", "zl", "zh"):
        signal(sem, here.to[link])
    mid = jnp.logical_not(here.end)

    @pl.when(mid)
    def _():
        signal(sem, here.to["in"])

    pl.semaphore_wait(sem, jnp.where(mid, 6, 5))


def blocks(g):
    return g.reshape(16, 2, g.shape[0] // 32, g.shape[1])


ANY, VMEM = pl.BlockSpec(memory_space=pl.ANY), pl.BlockSpec(memory_space=pltpu.VMEM)


def scattered(*g):
    g = [blocks(t) for t in g]

    def kernel(*refs):
        here = Place()
        total = Sum(here, refs[:3], refs[3:6], refs[6:])
        entry(here)
        total.start()
        for code in EVENTS:
            total.event(code)
        total.finish()

    return pl.pallas_call(
        kernel,
        out_shape=[jax.ShapeDtypeStruct(t.shape[2:], BF) for t in g],
        in_specs=[ANY] * 3,
        out_specs=[VMEM] * 3,
        scratch_shapes=sum_scratch(g),
        name="scattered",
        compiler_params=pltpu.CompilerParams(collective_id=1, has_side_effects=True, vmem_limit_bytes=56 << 20),
    )(*g)


def tiles(ref, width=256):
    def each(f):
        def one(i, carry):
            return f(pl.ds(pl.multiple_of(i * width, width), width), carry)

        return lambda carry: lax.fori_loop(0, ref.shape[-1] // width, one, carry)

    return each


def stepped(g1, g0, w, m, v):
    g0 = [blocks(t) for t in g0]
    count = sum(t.size for t in w)

    def kernel(*refs):
        g1, g0, w, m, v = (refs[i : i + 3] for i in range(0, 15, 3))
        new, new_m, new_v = (refs[i : i + 3] for i in range(15, 24, 3))
        r0, own_w, stage = (refs[i : i + 3] for i in range(24, 33, 3))
        norms, load, sends, link, core, nsent, ngot = refs[33:40]
        here = Place()
        total = Sum(here, g0, r0, refs[40:])
        entry(here)
        total.start()

        def rows_of(ref, p):
            rows = r0[p // 2].shape[0]
            return ref.at[p % 2, pl.ds(pl.multiple_of(here.me * rows, 8), rows), :]

        for p in range(6):
            pltpu.make_async_copy(rows_of(w[p // 2], p), own_w[p // 2].at[p % 2], load.at[p]).start()
        for code in EVENTS:
            total.event(code)

        squares = jnp.zeros((8, 128), F32)
        for ref in (*g1, *r0):
            def add(cols, so_far, ref=ref):
                g = ref[:, cols].astype(F32)
                g = (g * g).reshape(-1, 8, 2, 128)
                return so_far + jnp.sum(g[:, :, 0] + g[:, :, 1], 0)
            squares = tiles(ref)(add)(squares)
        squares = jnp.broadcast_to(jnp.sum(jnp.sum(squares, 0, keepdims=True), 1, keepdims=True), (8, 128))
        for k, to in enumerate(("core", "x", "y", "zl", "zh")):
            norms[k] = squares
            cp = pltpu.make_async_remote_copy(norms.at[k], norms.at[5 + k], nsent.at[k], ngot.at[k], device_id={"dp": here.to[to]}, device_id_type=MESH)
            cp.start()
            cp.wait()
            squares = squares + norms[5 + k]
        factor = jnp.minimum(1.0, 0.5 * lax.rsqrt(squares / count + 1e-30))[:1, :1]

        for p in range(6):
            a, n = p // 2, p % 2
            pltpu.make_async_copy(rows_of(w[a], p), own_w[a].at[n], load.at[p]).wait()
            g_ref = (g1 if n else r0)[a]

            def one(cols, _, a=a, n=n, g_ref=g_ref):
                g = g_ref[:, cols].astype(F32) * factor
                wide = own_w[a][n, :, cols].astype(F32)
                stage[a][n, :, cols], new_m[a][n, :, cols], new_v[a][n, :, cols] = adamw(wide, m[a][n, :, cols], v[a][n, :, cols], g)
                return 0

            tiles(g_ref)(one)(0)
            pltpu.make_async_copy(stage[a].at[n], rows_of(new[a], p), load.at[p]).start()
        for p in range(6):
            pltpu.make_async_copy(stage[p // 2].at[p % 2], rows_of(new[p // 2], p), load.at[p]).wait()
        gather_refs(here, new, sends, link, core)
        total.finish()

    state = [jax.ShapeDtypeStruct(t.shape, F32) for t in m]
    return pl.pallas_call(
        kernel,
        out_shape=[*(jax.ShapeDtypeStruct(t.shape, BF) for t in w), *state, *state],
        in_specs=[*[VMEM] * 3, *[ANY] * 6, *[VMEM] * 6],
        out_specs=[*[ANY] * 3, *[VMEM] * 6],
        scratch_shapes=[
            *(pltpu.VMEM(t.shape[2:], BF) for t in g0),
            *(pltpu.VMEM(t.shape, BF) for t in m),
            *(pltpu.VMEM(t.shape, BF) for t in m),
            pltpu.VMEM((10, 8, 128), F32),
            pltpu.SemaphoreType.DMA((6,)),
            pltpu.SemaphoreType.DMA((240,)),
            pltpu.SemaphoreType.DMA((6, 16)),
            pltpu.SemaphoreType.DMA((6, 16)),
            pltpu.SemaphoreType.DMA((5,)),
            pltpu.SemaphoreType.DMA((5,)),
            *sum_scratch(g0),
        ],
        name="stepped",
        compiler_params=pltpu.CompilerParams(collective_id=2, has_side_effects=True, vmem_limit_bytes=63 << 20),
    )(*g1, *g0, *w, *m, *v)


def dot(a, b, contract):
    return lax.dot_general(a, b, ((contract[:1], contract[1:]), ((), ())), preferred_element_type=F32)


def normed(h):
    wide = h.astype(F32)
    scale = lax.rsqrt(jnp.mean(wide**2, -1, keepdims=True) + 1e-6)
    return (wide * scale).astype(BF), scale


def gates(gate, up, by_hidden):
    by = by_hidden.astype(F32)
    sigmoid = jax.nn.sigmoid(gate)
    by_gate = by * up * (sigmoid * (1 + gate * (1 - sigmoid)))
    return by_gate.astype(BF), (by * gate * sigmoid).astype(BF)


def adamw(w, m, v, g):
    m = 0.9 * m + 0.1 * g
    v = 0.95 * v + 0.05 * g * g
    step = m * lax.rsqrt(v + 1e-8) + 0.1 * w
    return (w - 0.02 * step).astype(BF), m, v


def solution(mesh):
    def step(x, dy, *arrays):
        w, m, v = (arrays[i : i + 3] for i in (0, 3, 6))
        h, by = x[0], dy[0]
        layers, kept = w[0].shape[0], []
        for n in range(layers):
            a, scale = normed(h)
            gate, up = dot(a, w[0][n], (1, 0)), dot(a, w[1][n], (1, 0))
            hidden = (jax.nn.silu(gate) * up).astype(BF)
            kept.append((h, a, scale, gate, up, hidden))
            if n + 1 < layers:
                h = h + dot(hidden, w[2][n], (1, 0)).astype(BF)
        sums = [None] * layers
        for n in reversed(range(layers)):
            h, a, scale, gate, up, hidden = kept[n]
            by_down = dot(hidden, by, (0, 0)).astype(BF)
            by_hidden = dot(by, w[2][n], (1, 1)).astype(BF)
            by_gate, by_up = gates(gate, up, by_hidden)
            sums[n] = dot(a, by_gate, (0, 0)).astype(BF), dot(a, by_up, (0, 0)).astype(BF), by_down
            if n:
                by_a = dot(by_gate, w[0][n], (1, 1)).astype(BF) + dot(by_up, w[1][n], (1, 1)).astype(BF)
                wide, by_a = h.astype(F32), by_a.astype(F32)
                inner = jnp.mean(by_a * wide, -1, keepdims=True)
                by = by + (by_a * scale - wide * (scale**3 * inner)).astype(BF)
        return tuple(stepped(scattered(*sums[1]), sums[0], w, m, v))

    rows = P(None, "dp", None)
    return jax.shard_map(
        step,
        mesh=mesh,
        in_specs=(P(("rep", "dp")), P(("rep", "dp")), *(P(),) * 3, *(rows,) * 6),
        out_specs=(*(P("rep"),) * 3, *(P("rep", "dp", None),) * 6),
        check_vma=False,
    )
```

```python
import jax
import jax.numpy as jnp
from jax import lax
from jax.experimental import pallas as pl
from jax.experimental.pallas import tpu as pltpu
from jax.sharding import PartitionSpec as P

BF, F32 = jnp.bfloat16, jnp.float32
MESH = pl.DeviceIdType.MESH

ROUTE = ("A", "A", "B", "B", "Cx", "Cy")
END = (65, 36, 8, 81, 52, 24, 1, 84, 72, 17, 4, 40, 33, 20, 56, 49, 68, 88, 69, 73, 12, 44, 66, 37, 9, 85, 89, 28, 60, 82, 53, 92, 25, 5, 76, 41, 2, 21, 57, 18, 74, 45, 77, 70, 34, 13, 50, 93, 86, 90, 29, 61, 67, 38, 10, 6, 42, 58, 22, 78, 83, 54, 26, 94, 75, 71, 14, 46, 3, 19, 91, 62, 87, 30, 35, 79, 51, 95, 43, 7, 39, 11, 23, 59, 15, 47, 55, 27, 31, 63)
MID = (65, 66, 36, 8, 81, 82, 52, 24, 1, 2, 84, 72, 17, 18, 4, 40, 33, 34, 20, 56, 49, 50, 68, 88, 37, 9, 67, 69, 73, 38, 70, 74, 10, 12, 44, 53, 25, 83, 85, 89, 54, 86, 90, 26, 28, 60, 3, 92, 5, 19, 6, 76, 41, 42, 35, 51, 21, 57, 22, 58, 39, 11, 45, 13, 75, 46, 55, 27, 71, 77, 14, 78, 61, 29, 91, 93, 62, 94, 87, 30, 7, 43, 23, 59, 15, 47, 63, 31, 79, 95)

def at(x, y, z, c):
    return ((x * 2 + y) * 4 + z) * 2 + c

class Place:
    def __init__(self):
        me = lax.axis_index("dp")
        self.me = me
        self.x, self.y, self.z, self.c = x, y, z, c = me // 16, me // 8 % 2, me // 2 % 4, me % 2
        self.end = (z == 0) | (z == 3)
        low = z < 2
        self.planes = (z, jnp.where(z == 0, 1, jnp.where(z == 1, 0, jnp.where(z == 2, 3, 2))), jnp.where(low, 2, 1), jnp.where(low, 3, 0))
        inner = jnp.where(z == 0, 1, jnp.where(z == 1, 2, jnp.where(z == 2, 1, 2)))
        outer = jnp.where(low, 0, 3)
        self.own = {"x": x, "y": y, "zh": z // 2, "zl": z % 2, "c": c}
        self.to = {"zl": at(x, y, z + 1 - 2 * (z % 2), c), "zh": at(x, y, (z + 2) % 4, c), "x": at(1 - x, y, z, c), "y": at(x, 1 - y, z, c), "core": at(x, y, z, 1 - c), "in": at(x, y, inner, c), "out": at(x, y, outer, c)}

    def chip(self, dx, dy, s):
        x = 1 - self.x if dx else self.x
        y = 1 - self.y if dy else self.y
        return (x * 2 + y) * 4 + self.planes[s]

def onward(route, dx, dy, s, end):
    z = {0: ["in"] if end else ["out", "in"], 1: [] if end else ["in"], 2: [] if end else ["out"], 3: [] if end else ["out"]}[s]
    own = (dx, dy, s) == (0, 0, 0)
    first, second = ("x", "y") if route in ("A", "Cx") else ("y", "x")
    near = dy == 0 if first == "x" else dx == 0
    side = dx if first == "x" else dy
    if route in "AB":
        if own: return [first, *z, second]
        if not near: return []
        return [*z, second]
    if not near: return []
    if side: return [second]
    return [*z, first, second]

def signal(sem, device):
    pl.semaphore_signal(sem, inc=1, device_id={"dp": device}, device_id_type=MESH)

def START(end):
    zz = ["in"] if end else ["out", "in"]
    A, B, X, Y = (0, 1), (2, 3), (4,), (5,)
    o = [(p, l) for p in X + Y for l in zz]
    o += [(p, "x") for p in A] + [(p, "y") for p in B] + [(p, l) for p in A + B for l in zz]
    o += [(p, "x") for p in X] + [(p, "y") for p in Y] + [(p, "x") for p in B + Y] + [(p, "y") for p in A + X]
    return o + [(p, "core") for p in range(6)]

def gather_refs(here, outs, sends, link, core):
    def region(p, owner):
        ref = outs[p // 2]
        rows = ref.shape[1] // 32
        return ref.at[p % 2, pl.ds(pl.multiple_of(owner * rows, 8), rows), :]
    def run(end):
        started = []
        def send(p, chip, to):
            r = region(p, chip * 2 + here.c)
            cp = pltpu.make_async_remote_copy(r, r, sends.at[len(started)], (core if to == "core" else link).at[p, chip], device_id={"dp": here.to[to]}, device_id_type=MESH)
            started.append(cp)
            cp.start()
        def wait(p, owner, sem):
            pltpu.make_async_copy(region(p, owner), region(p, owner), sem).wait()
        mine = here.chip(0, 0, 0)
        for p, to in START(end): send(p, mine, to)
        for code in END if end else MID:
            p, dx, dy, s = code // 16, code // 8 % 2, code // 4 % 2, code % 4
            chip = here.chip(dx, dy, s)
            wait(p, chip * 2 + here.c, link.at[p, chip])
            for to in onward(ROUTE[p], dx, dy, s, end) + ["core"]: send(p, chip, to)
        def landed(chip, _):
            for p in range(6): wait(p, chip * 2 + 1 - here.c, core.at[p, chip])
            return 0
        lax.fori_loop(0, 16, landed, 0)
        for cp in started: cp.wait_send()
    @pl.when(here.end)
    def _(): run(True)
    @pl.when(jnp.logical_not(here.end))
    def _(): run(False)


XY, YX, ZX, ZY = ("x", "y", "zl", "zh"), ("y", "x", "zl", "zh"), ("zl", "x", "y", "zh"), ("zl", "y", "x", "zh")
WEIGHT = {"x": 8, "y": 4, "zh": 2, "zl": 1}
EVENTS = (1, 9, 17, 25, 33, 41, 2, 49, 10, 57, 18, 65, 26, 42, 34, 3, 66, 50, 4, 11, 5, 58, 19, 12, 27, 13, 35, 43, 28, 67, 36, 29, 51, 37, 59, 20, 44, 68, 52, 60, 21, 45, 69, 53, 61)
DUE = (2, 3, 4, 5, 6, 7, 8, 8, 9, 9, 9, 10, 12, 13, 13, 16, 17, 17, 18, 20, 20, 21, 22, 22, 23, 24, 24, 25, 25, 26, 26, 27, 28, 28, 28, 29, 29, 29, 30, 31, 32, 32, 33, 34, 34)


def streams(mats):
    out = []
    for m, ref in enumerate(mats):
        tiles = ref.shape[-1] // 128
        a, b = 128 * -(-tiles // 3), 128 * (-(-tiles // 3) + -(-(tiles - -(-tiles // 3)) // 2))
        out += [(m, 0, a, XY), (m, a, b - a, YX), (m, b, 128 * tiles - b, ZY if m % 2 else ZX)]
    return out


def sum_scratch(mats):
    out = []
    for m, _, w, _ in streams(mats):
        rows = mats[m].shape[-2]
        out += [pltpu.VMEM((2, 8, rows, w), BF), pltpu.VMEM((2, 8, rows, w), BF), pltpu.VMEM((15, rows, w), BF)]
    n = len(streams(mats))
    return [*out, pltpu.SemaphoreType.DMA((n,)), pltpu.SemaphoreType.DMA((n, 5)), pltpu.SemaphoreType.DMA((n, 5))]


class Sum:
    def __init__(self, here, mats, outs, scratch):
        self.here, self.mats, self.outs = here, mats, outs
        self.streams = streams(mats)
        n = len(self.streams)
        self.held = [scratch[3 * s : 3 * s + 3] for s in range(n)]
        self.local, self.sent, self.got = scratch[3 * n :]

    def parts(self, s, core, to):
        m, first, w, order = self.streams[s]
        ref, cols = self.mats[m], slice(first, first + w)
        if order[0] == "x":
            return [(ref.at[8 * h : 8 * h + 8, core, :, cols], to.at[h]) for h in (0, 1)]
        if order[0] == "y":
            return [(ref.at[8 * x + 4 * h : 8 * x + 4 * h + 4, core, :, cols], to.at[h, 4 * x : 4 * x + 4]) for h in (0, 1) for x in (0, 1)]
        return [(ref.at[b, core, :, cols], to.at[b % 2, b // 2]) for b in range(16)]

    def from_core(self, s):
        here = self.here
        return [
            pltpu.make_async_remote_copy(src, dst, self.sent.at[s, 0], self.got.at[s, 0], device_id={"dp": here.to["core"]}, device_id_type=MESH)
            for src, dst in self.parts(s, 1 - here.c, self.held[s][1])
        ]

    def whole(self, s, semaphore):
        ref = self.held[s][0]
        pltpu.make_async_copy(ref, ref, semaphore).wait()

    def copy(self, s, j):
        here = self.here
        own, core, came = self.held[s]
        order = self.streams[s][3]
        n = 16 >> j
        away = 1 - here.own[order[0]]
        src = own.at[away] if j == 1 else core.at[away, 8 - 2 * n : 8 - n]
        return pltpu.make_async_remote_copy(src, came.at[16 - 2 * n : 16 - n], self.sent.at[s, j], self.got.at[s, j], device_id={"dp": here.to[order[j - 1]]}, device_id_type=MESH)

    def start(self):
        for s in range(len(self.streams)):
            for cp in self.from_core(s):
                cp.start()
            for src, dst in self.parts(s, self.here.c, self.held[s][0]):
                pltpu.make_async_copy(src, dst, self.local.at[s]).start()

    def event(self, code):
        s, j = code // 8, code % 8
        m, first, w, order = self.streams[s]
        own, core, came = self.held[s]
        mine = self.here.own
        rest = [o for o in ("x", "y", "zh", "zl") if o != order[0]]
        weight = {o: 4 >> i for i, o in enumerate(rest)}
        if j == 1:
            self.whole(s, self.local.at[s])
            self.whole(s, self.got.at[s, 0])
        else:
            self.copy(s, j - 1).wait_recv()
        away = 0 if j == 5 else 1 - mine[order[j - 1]]
        half = away if j == 1 else mine[order[0]]

        def place(k):
            b = sum(mine[o] * weight[o] for o in order[1 : j - 1])
            if 1 < j < 5:
                b = b + away * weight[order[j - 1]]
            return b + sum(k // 2 ** (3 - i) % 2 * weight[order[i]] for i in range(j, 4))

        def block(k):
            b = place(k)
            total = own[half, b].astype(F32) + core[half, b].astype(F32)
            for i in range(1, j):
                if i == 1:
                    at_i = b
                else:
                    at_i = 16 - (32 >> i) + sum(mine[order[t]] * 2 ** (3 - t) for t in range(i, j - 1)) + k
                    if j < 5:
                        at_i = at_i + away * 2 ** (4 - j)
                total = total + came[at_i].astype(F32)
            return total.astype(BF)

        if j == 5:
            self.outs[m][:, first : first + w] = block(0)
            return
        n = 16 >> j

        def one(k, _):
            if j == 1:
                own[half, place(k)] = block(k)
            else:
                core[1 - mine[order[0]], 8 - 2 * n + k] = block(k)
            return 0

        lax.fori_loop(0, n, one, 0)
        self.copy(s, j).start()

    def finish(self):
        for s in range(len(self.streams)):
            self.whole(s, self.sent.at[s, 0])
            for j in range(1, 5):
                self.copy(s, j).wait_send()


def entry(here):
    sem = pltpu.get_barrier_semaphore()
    for link in ("x", "y", "core", "zl", "zh"):
        signal(sem, here.to[link])
    mid = jnp.logical_not(here.end)

    @pl.when(mid)
    def _():
        signal(sem, here.to["in"])

    pl.semaphore_wait(sem, jnp.where(mid, 6, 5))


def blocks(g):
    return g.reshape(16, 2, g.shape[0] // 32, g.shape[1])


ANY, VMEM = pl.BlockSpec(memory_space=pl.ANY), pl.BlockSpec(memory_space=pltpu.VMEM)


TILE = 256
PARAMS = {"vmem_limit_bytes": 63 << 20}


def once(shape):
    return pl.BlockSpec(shape, lambda t: (0,) * len(shape), pipeline_mode=pl.Buffered(1))


def prepared(h, by):
    tokens, d = h.shape
    rows = 512

    def kernel(h, by, a, a_t, by_t):
        a[...] = normed(h[...])
        a_t[...] = a[...].T
        by_t[...] = by[...].T

    short, tall = pl.BlockSpec((rows, d), lambda t: (t, 0)), pl.BlockSpec((d, rows), lambda t: (0, t))
    flat, turned = jax.ShapeDtypeStruct((tokens, d), BF), jax.ShapeDtypeStruct((d, tokens), BF)
    return pl.pallas_call(
        kernel,
        grid=(tokens // rows,),
        out_shape=[flat, turned, turned],
        in_specs=[short, short],
        out_specs=[short, tall, tall],
        name="prepared",
        compiler_params=pltpu.CompilerParams(**PARAMS),
    )(h, by)


def forward_up(n, a, w_gate, w_up, hidden):
    tokens, d = a.shape
    ff = w_gate.shape[2]

    def kernel(a, w_gate, w_up, gate, up, *hid):
        rows = 512
        for i in range(tokens // rows):
            at_i = slice(i * rows, (i + 1) * rows)
            g, u = dot(a[at_i, :], w_gate[...], (1, 0)), dot(a[at_i, :], w_up[...], (1, 0))
            gate[at_i, :], up[at_i, :] = g, u
            if hid:
                hid[0][at_i, :] = (jax.nn.silu(g) * u).astype(BF)

    tile, weight = pl.BlockSpec((tokens, TILE), lambda t: (0, t)), pl.BlockSpec((None, d, TILE), lambda t: (n, 0, t))
    return pl.pallas_call(
        kernel,
        grid=(ff // TILE,),
        out_shape=[jax.ShapeDtypeStruct((tokens, ff), t) for t in (F32, F32, BF)[: 2 + hidden]],
        in_specs=[once((tokens, d)), weight, weight],
        out_specs=[tile] * (2 + hidden),
        name="forward_up",
        compiler_params=pltpu.CompilerParams(**PARAMS),
    )(a, w_gate, w_up)


def forward_down(n, hidden, w_down, h):
    tokens, ff = hidden.shape
    d = h.shape[1]
    rows = 512

    def kernel(hidden, w_down, h, out, a, a_t):
        out[...] = h[...] + dot(hidden[...], w_down[...], (1, 0)).astype(BF)
        a[...] = normed(out[...])
        a_t[...] = a[...].T

    short, tall = pl.BlockSpec((rows, d), lambda t: (t, 0)), pl.BlockSpec((d, rows), lambda t: (0, t))
    flat, turned = jax.ShapeDtypeStruct((tokens, d), BF), jax.ShapeDtypeStruct((d, tokens), BF)
    return pl.pallas_call(
        kernel,
        grid=(tokens // rows,),
        out_shape=[flat, flat, turned],
        in_specs=[pl.BlockSpec((rows, ff), lambda t: (t, 0)), pl.BlockSpec((None, ff, d), lambda t: (n, 0, 0), pipeline_mode=pl.Buffered(1)), short],
        out_specs=[short, short, tall],
        name="forward_down",
        compiler_params=pltpu.CompilerParams(**PARAMS),
    )(hidden, w_down, h)


def of_tile(by, by_t, a_t, gate, up, w_down, hid, by_gate, by_up, by_w, between=lambda: None):
    rows = 512
    for i in range(by.shape[0] // rows):
        at_i = slice(i * rows, (i + 1) * rows)
        by_hidden = dot(by[at_i, :], w_down[...], (1, 1)).astype(BF).astype(F32)
        g, u = gate[at_i, :], up[at_i, :]
        sigmoid = jax.nn.sigmoid(g)
        silu = g * sigmoid
        hid[at_i, :] = (silu * u).astype(BF)
        by_up[at_i, :] = (by_hidden * silu).astype(BF)
        by_gate[at_i, :] = (by_hidden * u * (sigmoid + silu * (1 - sigmoid))).astype(BF)
    between()
    by_w[0][...] = dot(a_t[...], by_gate[...], (1, 0)).astype(BF)
    by_w[1][...] = dot(a_t[...], by_up[...], (1, 0)).astype(BF)
    by_w[2][...] = dot(by_t[...], hid[...], (1, 0)).T.astype(BF)


def backward(n, by, by_t, a_t, gate, up, w_down):
    tokens, d = by.shape
    ff = gate.shape[1]

    def kernel(by, by_t, a_t, gate, up, w_down, *refs):
        by_w, by_gate, by_up, hid = refs[:3], refs[3], refs[4], refs[5]
        of_tile(by, by_t, a_t, gate, up, w_down, hid, by_gate, by_up, by_w)

    tile = pl.BlockSpec((tokens, TILE), lambda t: (0, t))
    return pl.pallas_call(
        kernel,
        grid=(ff // TILE,),
        out_shape=[jax.ShapeDtypeStruct(s, BF) for s in ((d, ff), (d, ff), (ff, d), (tokens, ff), (tokens, ff))],
        in_specs=[once((tokens, d)), once((d, tokens)), once((d, tokens)), tile, tile, pl.BlockSpec((None, TILE, d), lambda t: (n, t, 0))],
        out_specs=[pl.BlockSpec((d, TILE), lambda t: (0, t))] * 2 + [pl.BlockSpec((TILE, d), lambda t: (t, 0)), tile, tile],
        scratch_shapes=[pltpu.VMEM((tokens, TILE), BF)],
        name="backward",
        compiler_params=pltpu.CompilerParams(**PARAMS),
    )(by, by_t, a_t, gate, up, w_down)


def backward_beside(g, n, by, by_t, a_t, gate, up, w_down):
    g = [blocks(t) for t in g]
    tokens, d = by.shape
    ff = gate.shape[1]
    steps = ff // TILE

    def kernel(*refs):
        by, by_t, a_t, gate, up, w_down = refs[:6]
        by_w, sums = refs[9:12], refs[12:15]
        hid, by_gate, by_up = refs[15:18]
        here = Place()
        total = Sum(here, refs[6:9], sums, refs[18:])
        step = pl.program_id(0)

        @pl.when(step == 0)
        def _():
            entry(here)
            total.start()

        def slot(part):
            for t in range(steps):
                due = [e for e, at_e in zip(EVENTS, DUE, strict=True) if min(at_e, 2 * steps - 1) == 2 * t + part]
                if due:
                    @pl.when(step == t)
                    def _(due=due):
                        for code in due:
                            total.event(code)

        of_tile(by, by_t, a_t, gate, up, w_down, hid, by_gate, by_up, by_w, lambda: slot(0))
        slot(1)

        @pl.when(step == steps - 1)
        def _():
            total.finish()

    tile = pl.BlockSpec((tokens, TILE), lambda t: (0, t))
    return pl.pallas_call(
        kernel,
        grid=(steps,),
        out_shape=[*(jax.ShapeDtypeStruct(s, BF) for s in ((d, ff), (d, ff), (ff, d))), *(jax.ShapeDtypeStruct(t.shape[2:], BF) for t in g)],
        in_specs=[once((tokens, d)), once((d, tokens)), once((d, tokens)), tile, tile, pl.BlockSpec((None, TILE, d), lambda t: (n, t, 0)), *[ANY] * 3],
        out_specs=[pl.BlockSpec((d, TILE), lambda t: (0, t))] * 2 + [pl.BlockSpec((TILE, d), lambda t: (t, 0))] + [once(t.shape[2:]) for t in g],
        scratch_shapes=[pltpu.VMEM((tokens, TILE), BF)] * 3 + sum_scratch(g),
        name="backward_beside",
        compiler_params=pltpu.CompilerParams(collective_id=1, has_side_effects=True, **PARAMS),
    )(by, by_t, a_t, gate, up, w_down, *g)


def backward_states(n, by_gate, by_up, w_gate, w_up, h, by):
    tokens, d = by.shape
    ff = by_gate.shape[1]
    rows = 512

    def kernel(by_gate, by_up, w_gate, w_up, h, by, out, out_t):
        by_a = dot(by_gate[...], w_gate[...], (1, 1)).astype(BF) + dot(by_up[...], w_up[...], (1, 1)).astype(BF)
        wide, by_a = h[...].astype(F32), by_a.astype(F32)
        scale = lax.rsqrt(jnp.mean(wide**2, -1, keepdims=True) + 1e-6)
        inner = jnp.mean(by_a * wide, -1, keepdims=True)
        new = by[...] + (by_a * scale - wide * (scale**3 * inner)).astype(BF)
        out[...] = new
        out_t[...] = new.T

    long, short = pl.BlockSpec((rows, ff), lambda t: (t, 0)), pl.BlockSpec((rows, d), lambda t: (t, 0))
    weight = pl.BlockSpec((None, d, ff), lambda t: (n, 0, 0), pipeline_mode=pl.Buffered(1))
    return pl.pallas_call(
        kernel,
        grid=(tokens // rows,),
        out_shape=[jax.ShapeDtypeStruct((tokens, d), BF), jax.ShapeDtypeStruct((d, tokens), BF)],
        in_specs=[long, long, weight, weight, short, short],
        out_specs=[short, pl.BlockSpec((d, rows), lambda t: (0, t))],
        name="backward_states",
        compiler_params=pltpu.CompilerParams(**PARAMS),
    )(by_gate, by_up, w_gate, w_up, h, by)


def tiles(ref, width=256):
    def each(f):
        def one(i, carry):
            return f(pl.ds(pl.multiple_of(i * width, width), width), carry)

        return lambda carry: lax.fori_loop(0, ref.shape[-1] // width, one, carry)

    return each


def stepped(g1, g0, w, m, v):
    g0 = [blocks(t) for t in g0]
    count = sum(t.size for t in w)

    def kernel(*refs):
        g1, g0, w, m, v = (refs[i : i + 3] for i in range(0, 15, 3))
        new, new_m, new_v = (refs[i : i + 3] for i in range(15, 24, 3))
        r0, own_w, stage = (refs[i : i + 3] for i in range(24, 33, 3))
        norms, load, sends, link, core, nsent, ngot = refs[33:40]
        here = Place()
        total = Sum(here, g0, r0, refs[40:])
        entry(here)
        total.start()

        def rows_of(ref, p):
            rows = r0[p // 2].shape[0]
            return ref.at[p % 2, pl.ds(pl.multiple_of(here.me * rows, 8), rows), :]

        for p in range(6):
            pltpu.make_async_copy(rows_of(w[p // 2], p), own_w[p // 2].at[p % 2], load.at[p]).start()
        for code in EVENTS:
            total.event(code)

        squares = jnp.zeros((8, 128), F32)
        for ref in (*g1, *r0):
            def add(cols, so_far, ref=ref):
                g = ref[:, cols].astype(F32)
                g = (g * g).reshape(-1, 8, 2, 128)
                return so_far + jnp.sum(g[:, :, 0] + g[:, :, 1], 0)
            squares = tiles(ref)(add)(squares)
        squares = jnp.broadcast_to(jnp.sum(jnp.sum(squares, 0, keepdims=True), 1, keepdims=True), (8, 128))
        for k, to in enumerate(("core", "x", "y", "zl", "zh")):
            norms[k] = squares
            cp = pltpu.make_async_remote_copy(norms.at[k], norms.at[5 + k], nsent.at[k], ngot.at[k], device_id={"dp": here.to[to]}, device_id_type=MESH)
            cp.start()
            cp.wait()
            squares = squares + norms[5 + k]
        factor = jnp.minimum(1.0, 0.5 * lax.rsqrt(squares / count + 1e-30))[:1, :1]

        for p in range(6):
            a, n = p // 2, p % 2
            pltpu.make_async_copy(rows_of(w[a], p), own_w[a].at[n], load.at[p]).wait()
            g_ref = (g1 if n else r0)[a]

            def one(cols, _, a=a, n=n, g_ref=g_ref):
                g = g_ref[:, cols].astype(F32) * factor
                wide = own_w[a][n, :, cols].astype(F32)
                stage[a][n, :, cols], new_m[a][n, :, cols], new_v[a][n, :, cols] = adamw(wide, m[a][n, :, cols], v[a][n, :, cols], g)
                return 0

            tiles(g_ref)(one)(0)
            pltpu.make_async_copy(stage[a].at[n], rows_of(new[a], p), load.at[p]).start()
        for p in range(6):
            pltpu.make_async_copy(stage[p // 2].at[p % 2], rows_of(new[p // 2], p), load.at[p]).wait()
        gather_refs(here, new, sends, link, core)
        total.finish()

    state = [jax.ShapeDtypeStruct(t.shape, F32) for t in m]
    return pl.pallas_call(
        kernel,
        out_shape=[*(jax.ShapeDtypeStruct(t.shape, BF) for t in w), *state, *state],
        in_specs=[*[VMEM] * 3, *[ANY] * 6, *[VMEM] * 6],
        out_specs=[*[ANY] * 3, *[VMEM] * 6],
        scratch_shapes=[
            *(pltpu.VMEM(t.shape[2:], BF) for t in g0),
            *(pltpu.VMEM(t.shape, BF) for t in m),
            *(pltpu.VMEM(t.shape, BF) for t in m),
            pltpu.VMEM((10, 8, 128), F32),
            pltpu.SemaphoreType.DMA((6,)),
            pltpu.SemaphoreType.DMA((240,)),
            pltpu.SemaphoreType.DMA((6, 16)),
            pltpu.SemaphoreType.DMA((6, 16)),
            pltpu.SemaphoreType.DMA((5,)),
            pltpu.SemaphoreType.DMA((5,)),
            *sum_scratch(g0),
        ],
        name="stepped",
        compiler_params=pltpu.CompilerParams(collective_id=2, has_side_effects=True, vmem_limit_bytes=63 << 20),
    )(*g1, *g0, *w, *m, *v)


def dot(a, b, contract):
    return lax.dot_general(a, b, ((contract[:1], contract[1:]), ((), ())), preferred_element_type=F32)


def normed(h):
    wide = h.astype(F32)
    return (wide * lax.rsqrt(jnp.mean(wide**2, -1, keepdims=True) + 1e-6)).astype(BF)


def adamw(w, m, v, g):
    m = 0.9 * m + 0.1 * g
    v = 0.95 * v + 0.05 * g * g
    step = m * lax.rsqrt(v + 1e-8) + 0.1 * w
    return (w - 0.02 * step).astype(BF), m, v


def solution(mesh):
    def step(x, dy, *arrays):
        w, m, v = (arrays[i : i + 3] for i in (0, 3, 6))
        h0, by = x[0], dy[0]
        a0, a0_t, by_t = prepared(h0, by)
        gate0, up0, hidden0 = forward_up(0, a0, w[0], w[1], True)
        h1, a1, a1_t = forward_down(0, hidden0, w[2], h0)
        gate1, up1 = forward_up(1, a1, w[0], w[1], False)
        *g1, by_gate, by_up = backward(1, by, by_t, a1_t, gate1, up1, w[2])
        by, by_t = backward_states(1, by_gate, by_up, w[0], w[1], h1, by)
        both = backward_beside(g1, 0, by, by_t, a0_t, gate0, up0, w[2])
        return tuple(stepped(both[3:], both[:3], w, m, v))

    rows = P(None, "dp", None)
    return jax.shard_map(
        step,
        mesh=mesh,
        in_specs=(P(("rep", "dp")), P(("rep", "dp")), *(P(),) * 3, *(rows,) * 6),
        out_specs=(*(P("rep"),) * 3, *(P("rep", "dp", None),) * 6),
        check_vma=False,
    )
```

```python
import jax
import jax.numpy as jnp
from jax import lax
from jax.experimental import pallas as pl
from jax.experimental.pallas import tpu as pltpu
from jax.sharding import PartitionSpec as P

BF, F32 = jnp.bfloat16, jnp.float32
MESH = pl.DeviceIdType.MESH

ROUTE = ("A", "A", "B", "B", "Cx", "Cy")
END = (65, 36, 8, 81, 52, 24, 1, 84, 72, 17, 4, 40, 33, 20, 56, 49, 68, 88, 69, 73, 12, 44, 66, 37, 9, 85, 89, 28, 60, 82, 53, 92, 25, 5, 76, 41, 2, 21, 57, 18, 74, 45, 77, 70, 34, 13, 50, 93, 86, 90, 29, 61, 67, 38, 10, 6, 42, 58, 22, 78, 83, 54, 26, 94, 75, 71, 14, 46, 3, 19, 91, 62, 87, 30, 35, 79, 51, 95, 43, 7, 39, 11, 23, 59, 15, 47, 55, 27, 31, 63)
MID = (65, 66, 36, 8, 81, 82, 52, 24, 1, 2, 84, 72, 17, 18, 4, 40, 33, 34, 20, 56, 49, 50, 68, 88, 37, 9, 67, 69, 73, 38, 70, 74, 10, 12, 44, 53, 25, 83, 85, 89, 54, 86, 90, 26, 28, 60, 3, 92, 5, 19, 6, 76, 41, 42, 35, 51, 21, 57, 22, 58, 39, 11, 45, 13, 75, 46, 55, 27, 71, 77, 14, 78, 61, 29, 91, 93, 62, 94, 87, 30, 7, 43, 23, 59, 15, 47, 63, 31, 79, 95)

def at(x, y, z, c):
    return ((x * 2 + y) * 4 + z) * 2 + c

class Place:
    def __init__(self):
        me = lax.axis_index("dp")
        self.me = me
        self.x, self.y, self.z, self.c = x, y, z, c = me // 16, me // 8 % 2, me // 2 % 4, me % 2
        self.end = (z == 0) | (z == 3)
        low = z < 2
        self.planes = (z, jnp.where(z == 0, 1, jnp.where(z == 1, 0, jnp.where(z == 2, 3, 2))), jnp.where(low, 2, 1), jnp.where(low, 3, 0))
        inner = jnp.where(z == 0, 1, jnp.where(z == 1, 2, jnp.where(z == 2, 1, 2)))
        outer = jnp.where(low, 0, 3)
        self.own = {"x": x, "y": y, "zh": z // 2, "zl": z % 2, "c": c}
        self.to = {"zl": at(x, y, z + 1 - 2 * (z % 2), c), "zh": at(x, y, (z + 2) % 4, c), "x": at(1 - x, y, z, c), "y": at(x, 1 - y, z, c), "core": at(x, y, z, 1 - c), "in": at(x, y, inner, c), "out": at(x, y, outer, c)}

    def chip(self, dx, dy, s):
        x = 1 - self.x if dx else self.x
        y = 1 - self.y if dy else self.y
        return (x * 2 + y) * 4 + self.planes[s]

def onward(route, dx, dy, s, end):
    z = {0: ["in"] if end else ["out", "in"], 1: [] if end else ["in"], 2: [] if end else ["out"], 3: [] if end else ["out"]}[s]
    own = (dx, dy, s) == (0, 0, 0)
    first, second = ("x", "y") if route in ("A", "Cx") else ("y", "x")
    near = dy == 0 if first == "x" else dx == 0
    side = dx if first == "x" else dy
    if route in "AB":
        if own: return [first, *z, second]
        if not near: return []
        return [*z, second]
    if not near: return []
    if side: return [second]
    return [*z, first, second]

def signal(sem, device):
    pl.semaphore_signal(sem, inc=1, device_id={"dp": device}, device_id_type=MESH)

def START(end):
    zz = ["in"] if end else ["out", "in"]
    A, B, X, Y = (0, 1), (2, 3), (4,), (5,)
    o = [(p, l) for p in X + Y for l in zz]
    o += [(p, "x") for p in A] + [(p, "y") for p in B] + [(p, l) for p in A + B for l in zz]
    o += [(p, "x") for p in X] + [(p, "y") for p in Y] + [(p, "x") for p in B + Y] + [(p, "y") for p in A + X]
    return o + [(p, "core") for p in range(6)]

def gather_refs(here, outs, sends, link, core):
    def region(p, owner):
        ref = outs[p // 2]
        rows = ref.shape[1] // 32
        return ref.at[p % 2, pl.ds(pl.multiple_of(owner * rows, 8), rows), :]
    def run(end):
        started = []
        def send(p, chip, to):
            r = region(p, chip * 2 + here.c)
            cp = pltpu.make_async_remote_copy(r, r, sends.at[len(started)], (core if to == "core" else link).at[p, chip], device_id={"dp": here.to[to]}, device_id_type=MESH)
            started.append(cp)
            cp.start()
        def wait(p, owner, sem):
            pltpu.make_async_copy(region(p, owner), region(p, owner), sem).wait()
        mine = here.chip(0, 0, 0)
        for p, to in START(end): send(p, mine, to)
        for code in END if end else MID:
            p, dx, dy, s = code // 16, code // 8 % 2, code // 4 % 2, code % 4
            chip = here.chip(dx, dy, s)
            wait(p, chip * 2 + here.c, link.at[p, chip])
            for to in onward(ROUTE[p], dx, dy, s, end) + ["core"]: send(p, chip, to)
        def landed(chip, _):
            for p in range(6): wait(p, chip * 2 + 1 - here.c, core.at[p, chip])
            return 0
        lax.fori_loop(0, 16, landed, 0)
        for cp in started: cp.wait_send()
    @pl.when(here.end)
    def _(): run(True)
    @pl.when(jnp.logical_not(here.end))
    def _(): run(False)


STREAMS = (
    (0, 0, 640, ('zl', 'zh', 'x', 'y')),
    (1, 0, 768, ('x', 'zl', 'y', 'zh')),
    (1, 768, 1024, ('y', 'x', 'zl', 'zh')),
    (2, 0, 384, ('zl', 'x', 'y', 'zh')),
    (2, 384, 384, ('x', 'zl', 'y', 'zh')),
    (0, 640, 1664, ('y', 'zl', 'zh', 'x')),
    (0, 2304, 1024, ('y', 'zl', 'x', 'zh')),
    (1, 1792, 1536, ('x', 'y', 'zl', 'zh')),
    (2, 768, 256, ('x', 'y', 'zl', 'zh')),
)
EVENTS = (1, 9, 17, 25, 33, 2, 10, 41, 49, 18, 57, 65, 26, 34, 3, 11, 19, 42, 35, 20, 50, 58, 12, 43, 21, 36, 51, 66, 13, 59, 44, 27, 37, 67, 4, 60, 52, 68, 28, 45, 5, 61, 53, 69, 29)
DUE = (0, 1, 1, 2, 2, 2, 3, 3, 3, 4, 4, 5, 5, 5, 6, 6, 6, 7, 7, 8, 9, 9, 10, 10, 10, 10, 11, 11, 11, 12, 12, 12, 12, 13, 13, 13, 13, 13, 13, 14, 14, 14, 14, 14, 15)


def sum_scratch(mats):
    out = []
    for m, _, w, _ in STREAMS:
        rows = mats[m].shape[-2]
        out += [pltpu.VMEM((2, 8, rows, w), BF), pltpu.VMEM((2, 8, rows, w), BF), pltpu.VMEM((15, rows, w), BF)]
    n = len(STREAMS)
    return [*out, pltpu.SemaphoreType.DMA((n,)), pltpu.SemaphoreType.DMA((n, 5)), pltpu.SemaphoreType.DMA((n, 5))]


class Sum:
    def __init__(self, here, mats, outs, scratch):
        self.here, self.mats, self.outs = here, mats, outs
        self.streams = STREAMS
        n = len(self.streams)
        self.held = [scratch[3 * s : 3 * s + 3] for s in range(n)]
        self.local, self.sent, self.got = scratch[3 * n :]

    def parts(self, s, core, to):
        m, first, w, order = self.streams[s]
        ref, cols = self.mats[m], slice(first, first + w)
        if order[0] == "x":
            return [(ref.at[8 * h : 8 * h + 8, core, :, cols], to.at[h]) for h in (0, 1)]
        if order[0] == "y":
            return [(ref.at[8 * x + 4 * h : 8 * x + 4 * h + 4, core, :, cols], to.at[h, 4 * x : 4 * x + 4]) for h in (0, 1) for x in (0, 1)]
        return [(ref.at[b, core, :, cols], to.at[b % 2, b // 2]) for b in range(16)]

    def from_core(self, s):
        here = self.here
        return [
            pltpu.make_async_remote_copy(src, dst, self.sent.at[s, 0], self.got.at[s, 0], device_id={"dp": here.to["core"]}, device_id_type=MESH)
            for src, dst in self.parts(s, 1 - here.c, self.held[s][1])
        ]

    def whole(self, s, semaphore):
        ref = self.held[s][0]
        pltpu.make_async_copy(ref, ref, semaphore).wait()

    def copy(self, s, j):
        here = self.here
        own, core, came = self.held[s]
        order = self.streams[s][3]
        n = 16 >> j
        away = 1 - here.own[order[0]]
        src = own.at[away] if j == 1 else core.at[away, 8 - 2 * n : 8 - n]
        return pltpu.make_async_remote_copy(src, came.at[16 - 2 * n : 16 - n], self.sent.at[s, j], self.got.at[s, j], device_id={"dp": here.to[order[j - 1]]}, device_id_type=MESH)

    def start(self):
        for s in range(len(self.streams)):
            for cp in self.from_core(s):
                cp.start()
            for src, dst in self.parts(s, self.here.c, self.held[s][0]):
                pltpu.make_async_copy(src, dst, self.local.at[s]).start()

    def event(self, code):
        s, j = code // 8, code % 8
        m, first, w, order = self.streams[s]
        own, core, came = self.held[s]
        mine = self.here.own
        rest = [o for o in ("x", "y", "zh", "zl") if o != order[0]]
        weight = {o: 4 >> i for i, o in enumerate(rest)}
        if j == 1:
            self.whole(s, self.local.at[s])
            self.whole(s, self.got.at[s, 0])
        else:
            self.copy(s, j - 1).wait_recv()
        away = 0 if j == 5 else 1 - mine[order[j - 1]]
        half = away if j == 1 else mine[order[0]]

        def place(k):
            b = sum(mine[o] * weight[o] for o in order[1 : j - 1])
            if 1 < j < 5:
                b = b + away * weight[order[j - 1]]
            return b + sum(k // 2 ** (3 - i) % 2 * weight[order[i]] for i in range(j, 4))

        def block(k):
            b = place(k)
            total = own[half, b].astype(F32) + core[half, b].astype(F32)
            for i in range(1, j):
                if i == 1:
                    at_i = b
                else:
                    at_i = 16 - (32 >> i) + sum(mine[order[t]] * 2 ** (3 - t) for t in range(i, j - 1)) + k
                    if j < 5:
                        at_i = at_i + away * 2 ** (4 - j)
                total = total + came[at_i].astype(F32)
            return total.astype(BF)

        if j == 5:
            self.outs[m][:, first : first + w] = block(0)
            return
        n = 16 >> j

        def one(k, _):
            if j == 1:
                own[half, place(k)] = block(k)
            else:
                core[1 - mine[order[0]], 8 - 2 * n + k] = block(k)
            return 0

        lax.fori_loop(0, n, one, 0)
        self.copy(s, j).start()

    def finish(self):
        for s in range(len(self.streams)):
            self.whole(s, self.sent.at[s, 0])
            for j in range(1, 5):
                self.copy(s, j).wait_send()


def entry(here):
    sem = pltpu.get_barrier_semaphore()
    for link in ("x", "y", "core", "zl", "zh"):
        signal(sem, here.to[link])
    mid = jnp.logical_not(here.end)

    @pl.when(mid)
    def _():
        signal(sem, here.to["in"])

    pl.semaphore_wait(sem, jnp.where(mid, 6, 5))


def blocks(g):
    return g.reshape(16, 2, g.shape[0] // 32, g.shape[1])


ANY, VMEM = pl.BlockSpec(memory_space=pl.ANY), pl.BlockSpec(memory_space=pltpu.VMEM)


TILE = 256
PARAMS = {"vmem_limit_bytes": 63 << 20}


def once(shape):
    return pl.BlockSpec(shape, lambda t: (0,) * len(shape), pipeline_mode=pl.Buffered(1))


def prepared(h, by):
    tokens, d = h.shape
    rows = 512

    def kernel(h, by, a, a_t, by_t):
        a[...] = normed(h[...])
        a_t[...] = a[...].T
        by_t[...] = by[...].T

    short, tall = pl.BlockSpec((rows, d), lambda t: (t, 0)), pl.BlockSpec((d, rows), lambda t: (0, t))
    flat, turned = jax.ShapeDtypeStruct((tokens, d), BF), jax.ShapeDtypeStruct((d, tokens), BF)
    return pl.pallas_call(
        kernel,
        grid=(tokens // rows,),
        out_shape=[flat, turned, turned],
        in_specs=[short, short],
        out_specs=[short, tall, tall],
        name="prepared",
        compiler_params=pltpu.CompilerParams(**PARAMS),
    )(h, by)


def forward_up(n, a, w_gate, w_up, hidden):
    tokens, d = a.shape
    ff = w_gate.shape[2]

    def kernel(a, w_gate, w_up, gate, up, *hid):
        rows = 512
        for i in range(tokens // rows):
            at_i = slice(i * rows, (i + 1) * rows)
            g, u = dot(a[at_i, :], w_gate[...], (1, 0)), dot(a[at_i, :], w_up[...], (1, 0))
            gate[at_i, :], up[at_i, :] = g, u
            if hid:
                hid[0][at_i, :] = (jax.nn.silu(g) * u).astype(BF)

    tile, weight = pl.BlockSpec((tokens, TILE), lambda t: (0, t)), pl.BlockSpec((None, d, TILE), lambda t: (n, 0, t))
    return pl.pallas_call(
        kernel,
        grid=(ff // TILE,),
        out_shape=[jax.ShapeDtypeStruct((tokens, ff), t) for t in (F32, F32, BF)[: 2 + hidden]],
        in_specs=[once((tokens, d)), weight, weight],
        out_specs=[tile] * (2 + hidden),
        name="forward_up",
        compiler_params=pltpu.CompilerParams(**PARAMS),
    )(a, w_gate, w_up)


def forward_down(n, hidden, w_down, h):
    tokens, ff = hidden.shape
    d = h.shape[1]
    rows = 512

    def kernel(hidden, w_down, h, out, a, a_t):
        out[...] = h[...] + dot(hidden[...], w_down[...], (1, 0)).astype(BF)
        a[...] = normed(out[...])
        a_t[...] = a[...].T

    short, tall = pl.BlockSpec((rows, d), lambda t: (t, 0)), pl.BlockSpec((d, rows), lambda t: (0, t))
    flat, turned = jax.ShapeDtypeStruct((tokens, d), BF), jax.ShapeDtypeStruct((d, tokens), BF)
    return pl.pallas_call(
        kernel,
        grid=(tokens // rows,),
        out_shape=[flat, flat, turned],
        in_specs=[pl.BlockSpec((rows, ff), lambda t: (t, 0)), pl.BlockSpec((None, ff, d), lambda t: (n, 0, 0), pipeline_mode=pl.Buffered(1)), short],
        out_specs=[short, short, tall],
        name="forward_down",
        compiler_params=pltpu.CompilerParams(**PARAMS),
    )(hidden, w_down, h)


def of_tile(by, by_t, a_t, gate, up, w_down, hid, by_gate, by_up, by_w, between=lambda: None):
    rows = 512
    for i in range(by.shape[0] // rows):
        at_i = slice(i * rows, (i + 1) * rows)
        by_hidden = dot(by[at_i, :], w_down[...], (1, 1)).astype(BF).astype(F32)
        g, u = gate[at_i, :], up[at_i, :]
        sigmoid = jax.nn.sigmoid(g)
        silu = g * sigmoid
        hid[at_i, :] = (silu * u).astype(BF)
        by_up[at_i, :] = (by_hidden * silu).astype(BF)
        by_gate[at_i, :] = (by_hidden * u * (sigmoid + silu * (1 - sigmoid))).astype(BF)
    by_w[0][...] = dot(a_t[...], by_gate[...], (1, 0)).astype(BF)
    by_w[1][...] = dot(a_t[...], by_up[...], (1, 0)).astype(BF)
    by_w[2][...] = dot(by_t[...], hid[...], (1, 0)).T.astype(BF)
    between()


def backward(n, by, by_t, a_t, gate, up, w_down):
    tokens, d = by.shape
    ff = gate.shape[1]

    def kernel(by, by_t, a_t, gate, up, w_down, *refs):
        by_w, by_gate, by_up, hid = refs[:3], refs[3], refs[4], refs[5]
        of_tile(by, by_t, a_t, gate, up, w_down, hid, by_gate, by_up, by_w)

    tile = pl.BlockSpec((tokens, TILE), lambda t: (0, t))
    return pl.pallas_call(
        kernel,
        grid=(ff // TILE,),
        out_shape=[jax.ShapeDtypeStruct(s, BF) for s in ((d, ff), (d, ff), (ff, d), (tokens, ff), (tokens, ff))],
        in_specs=[once((tokens, d)), once((d, tokens)), once((d, tokens)), tile, tile, pl.BlockSpec((None, TILE, d), lambda t: (n, t, 0))],
        out_specs=[pl.BlockSpec((d, TILE), lambda t: (0, t))] * 2 + [pl.BlockSpec((TILE, d), lambda t: (t, 0)), tile, tile],
        scratch_shapes=[pltpu.VMEM((tokens, TILE), BF)],
        name="backward",
        compiler_params=pltpu.CompilerParams(**PARAMS),
    )(by, by_t, a_t, gate, up, w_down)


def backward_beside(g, n, by, by_t, a_t, gate, up, w_down):
    g = [blocks(t) for t in g]
    tokens, d = by.shape
    ff = gate.shape[1]
    steps = ff // TILE

    def kernel(*refs):
        by, by_t, a_t, gate, up, w_down = refs[:6]
        by_w, sums = refs[9:12], refs[12:15]
        hid, by_gate, by_up = refs[15:18]
        here = Place()
        total = Sum(here, refs[6:9], sums, refs[18:])
        step = pl.program_id(0)

        @pl.when(step == 0)
        def _():
            entry(here)
            total.start()

        def slot():
            for t in range(steps):
                due = [e for e, at_e in zip(EVENTS, DUE, strict=True) if min(at_e, steps - 1) == t]
                if due:
                    @pl.when(step == t)
                    def _(due=due):
                        for code in due:
                            total.event(code)

        of_tile(by, by_t, a_t, gate, up, w_down, hid, by_gate, by_up, by_w, slot)

        @pl.when(step == steps - 1)
        def _():
            total.finish()

    tile = pl.BlockSpec((tokens, TILE), lambda t: (0, t))
    return pl.pallas_call(
        kernel,
        grid=(steps,),
        out_shape=[*(jax.ShapeDtypeStruct(s, BF) for s in ((d, ff), (d, ff), (ff, d))), *(jax.ShapeDtypeStruct(t.shape[2:], BF) for t in g)],
        in_specs=[once((tokens, d)), once((d, tokens)), once((d, tokens)), tile, tile, pl.BlockSpec((None, TILE, d), lambda t: (n, t, 0)), *[ANY] * 3],
        out_specs=[pl.BlockSpec((d, TILE), lambda t: (0, t))] * 2 + [pl.BlockSpec((TILE, d), lambda t: (t, 0))] + [once(t.shape[2:]) for t in g],
        scratch_shapes=[pltpu.VMEM((tokens, TILE), BF)] * 3 + sum_scratch(g),
        name="backward_beside",
        compiler_params=pltpu.CompilerParams(collective_id=1, has_side_effects=True, **PARAMS),
    )(by, by_t, a_t, gate, up, w_down, *g)


def backward_states(n, by_gate, by_up, w_gate, w_up, h, by):
    tokens, d = by.shape
    ff = by_gate.shape[1]
    rows = 512

    def kernel(by_gate, by_up, w_gate, w_up, h, by, out, out_t):
        by_a = dot(by_gate[...], w_gate[...], (1, 1)).astype(BF) + dot(by_up[...], w_up[...], (1, 1)).astype(BF)
        wide, by_a = h[...].astype(F32), by_a.astype(F32)
        scale = lax.rsqrt(jnp.mean(wide**2, -1, keepdims=True) + 1e-6)
        inner = jnp.mean(by_a * wide, -1, keepdims=True)
        new = by[...] + (by_a * scale - wide * (scale**3 * inner)).astype(BF)
        out[...] = new
        out_t[...] = new.T

    long, short = pl.BlockSpec((rows, ff), lambda t: (t, 0)), pl.BlockSpec((rows, d), lambda t: (t, 0))
    weight = pl.BlockSpec((None, d, ff), lambda t: (n, 0, 0), pipeline_mode=pl.Buffered(1))
    return pl.pallas_call(
        kernel,
        grid=(tokens // rows,),
        out_shape=[jax.ShapeDtypeStruct((tokens, d), BF), jax.ShapeDtypeStruct((d, tokens), BF)],
        in_specs=[long, long, weight, weight, short, short],
        out_specs=[short, pl.BlockSpec((d, rows), lambda t: (0, t))],
        name="backward_states",
        compiler_params=pltpu.CompilerParams(**PARAMS),
    )(by_gate, by_up, w_gate, w_up, h, by)


def tiles(ref, width=256):
    def each(f):
        def one(i, carry):
            return f(pl.ds(pl.multiple_of(i * width, width), width), carry)

        return lambda carry: lax.fori_loop(0, ref.shape[-1] // width, one, carry)

    return each


def clipping(g1, g0, count):
    g0 = [blocks(t) for t in g0]

    def kernel(*refs):
        g1, g0, r0, factor = refs[:3], refs[3:6], refs[6:9], refs[9]
        norms, nsent, ngot = refs[10:13]
        here = Place()
        total = Sum(here, g0, r0, refs[13:])
        entry(here)
        total.start()
        for code in EVENTS:
            total.event(code)
        squares = jnp.zeros((8, 128), F32)
        for ref in (*g1, *r0):

            def add(cols, so_far, ref=ref):
                g = ref[:, cols].astype(F32)
                g = (g * g).reshape(-1, 8, 2, 128)
                return so_far + jnp.sum(g[:, :, 0] + g[:, :, 1], 0)

            squares = tiles(ref)(add)(squares)
        squares = jnp.broadcast_to(jnp.sum(jnp.sum(squares, 0, keepdims=True), 1, keepdims=True), (8, 128))
        for k, to in enumerate(("core", "x", "y", "zl", "zh")):
            norms[k] = squares
            cp = pltpu.make_async_remote_copy(norms.at[k], norms.at[5 + k], nsent.at[k], ngot.at[k], device_id={"dp": here.to[to]}, device_id_type=MESH)
            cp.start()
            cp.wait()
            squares = squares + norms[5 + k]
        factor[...] = jnp.minimum(1.0, 0.5 * lax.rsqrt(squares / count + 1e-30))
        total.finish()

    return pl.pallas_call(
        kernel,
        out_shape=[*(jax.ShapeDtypeStruct(t.shape[2:], BF) for t in g0), jax.ShapeDtypeStruct((8, 128), F32)],
        in_specs=[*[VMEM] * 3, *[ANY] * 3],
        out_specs=[VMEM] * 4,
        scratch_shapes=[pltpu.VMEM((10, 8, 128), F32), pltpu.SemaphoreType.DMA((5,)), pltpu.SemaphoreType.DMA((5,)), *sum_scratch(g0)],
        name="clipping",
        compiler_params=pltpu.CompilerParams(collective_id=2, has_side_effects=True, vmem_limit_bytes=48 << 20),
    )(*g1, *g0)


def stepped(g1, g0, factor, w, m, v):
    def kernel(*refs):
        g1, g0, factor, w, m, v = refs[:3], refs[3:6], refs[6][:1, :1], refs[7:10], refs[10:13], refs[13:16]
        new, new_m, new_v, own_w, load = refs[16:19], refs[19:22], refs[22:25], refs[25:28], refs[28]
        me = lax.axis_index("dp")

        def own(p):
            rows = g0[p // 2].shape[0]
            src = w[p // 2].at[p % 2, pl.ds(pl.multiple_of(me * rows, 8), rows), :]
            return pltpu.make_async_copy(src, own_w[p // 2].at[p % 2], load.at[p])

        for p in range(6):
            own(p).start()
        for p in range(6):
            a, n = p // 2, p % 2
            own(p).wait()
            g_ref = (g1 if n else g0)[a]

            def one(cols, _, a=a, n=n, g_ref=g_ref):
                g = g_ref[:, cols].astype(F32) * factor
                wide = own_w[a][n, :, cols].astype(F32)
                new[a][n, :, cols], new_m[a][n, :, cols], new_v[a][n, :, cols] = adamw(wide, m[a][n, :, cols], v[a][n, :, cols], g)
                return 0

            tiles(g_ref)(one)(0)

    state = [jax.ShapeDtypeStruct(t.shape, F32) for t in m]
    return pl.pallas_call(
        kernel,
        out_shape=[*(jax.ShapeDtypeStruct(t.shape, BF) for t in m), *state, *state],
        in_specs=[*[VMEM] * 7, *[ANY] * 3, *[VMEM] * 6],
        out_specs=[VMEM] * 9,
        scratch_shapes=[*(pltpu.VMEM(t.shape, BF) for t in m), pltpu.SemaphoreType.DMA((6,))],
        name="stepped",
        compiler_params=pltpu.CompilerParams(vmem_limit_bytes=24 << 20),
    )(*g1, *g0, factor, *w, *m, *v)


def gathered(*own):
    def kernel(*refs):
        own, outs, stage = refs[:3], refs[3:6], refs[6:9]
        load, sends, link, core = refs[9:]
        here = Place()

        def into(p):
            return pltpu.make_async_copy(own[p // 2].at[p % 2], stage[p // 2].at[p % 2], load.at[p])

        def out(p):
            rows = stage[p // 2].shape[1]
            return pltpu.make_async_copy(stage[p // 2].at[p % 2], outs[p // 2].at[p % 2, pl.ds(pl.multiple_of(here.me * rows, 8), rows), :], load.at[p])

        for p in range(6):
            into(p).start()
        entry(here)
        for p in range(6):
            into(p).wait()
            out(p).start()
        for p in range(6):
            out(p).wait()
        gather_refs(here, outs, sends, link, core)

    return pl.pallas_call(
        kernel,
        out_shape=[jax.ShapeDtypeStruct((2, 32 * t.shape[1], t.shape[2]), BF) for t in own],
        in_specs=[ANY] * 3,
        out_specs=[ANY] * 3,
        scratch_shapes=[
            *(pltpu.VMEM(t.shape, BF) for t in own),
            pltpu.SemaphoreType.DMA((6,)),
            pltpu.SemaphoreType.DMA((240,)),
            pltpu.SemaphoreType.DMA((6, 16)),
            pltpu.SemaphoreType.DMA((6, 16)),
        ],
        name="gathered",
        compiler_params=pltpu.CompilerParams(collective_id=3, has_side_effects=True, vmem_limit_bytes=8 << 20),
    )(*own)


def dot(a, b, contract):
    return lax.dot_general(a, b, ((contract[:1], contract[1:]), ((), ())), preferred_element_type=F32)


def normed(h):
    wide = h.astype(F32)
    return (wide * lax.rsqrt(jnp.mean(wide**2, -1, keepdims=True) + 1e-6)).astype(BF)


def adamw(w, m, v, g):
    m = 0.9 * m + 0.1 * g
    v = 0.95 * v + 0.05 * g * g
    step = m * lax.rsqrt(v + 1e-8) + 0.1 * w
    return (w - 0.02 * step).astype(BF), m, v


def solution(mesh):
    def step(x, dy, *arrays):
        w, m, v = (arrays[i : i + 3] for i in (0, 3, 6))
        h0, by = x[0], dy[0]
        a0, a0_t, by_t = prepared(h0, by)
        gate0, up0, hidden0 = forward_up(0, a0, w[0], w[1], True)
        h1, a1, a1_t = forward_down(0, hidden0, w[2], h0)
        gate1, up1 = forward_up(1, a1, w[0], w[1], False)
        *g1, by_gate, by_up = backward(1, by, by_t, a1_t, gate1, up1, w[2])
        by, by_t = backward_states(1, by_gate, by_up, w[0], w[1], h1, by)
        both = backward_beside(g1, 0, by, by_t, a0_t, gate0, up0, w[2])
        *g0, factor = clipping(both[3:], both[:3], sum(t.size for t in w))
        new = stepped(both[3:], g0, factor, w, m, v)
        return (*gathered(*new[:3]), *new[3:])

    rows = P(None, "dp", None)
    return jax.shard_map(
        step,
        mesh=mesh,
        in_specs=(P(("rep", "dp")), P(("rep", "dp")), *(P(),) * 3, *(rows,) * 6),
        out_specs=(*(P("rep"),) * 3, *(P("rep", "dp", None),) * 6),
        check_vma=False,
    )
```
